32 devices in a mesh: depth: 4 (over y, core), blk: 8 (over z, x).
Axes of the slice: x: 2, y: 2, z: 4, core: 2. Of those that a mesh axis runs over, the one named last changes fastest.
Arguments:
- jacobian: bfloat16 [96, 16384], P(('depth', 'blk')), may hold values from -6 to 6
- gain_inverse: bfloat16 [16384, 16384], P('depth', 'blk'), may hold values from -0.00024414062 to 0.00048828125, as said below
- variance: float32 [96], P(('depth', 'blk')), may hold values from 2 to 12
Outputs:
- omega_diag: float32 [96], P(('depth', 'blk'))
The draws below stay inside these ranges and needn't reach their ends.
Inputs may be any that keep to these rules, and one draw needn't show every extreme that they name: gain_inverse is symmetric and positive definite.
All inputs are finite; a program needn't handle non-finite values.
Results may differ from the reference program's by a relative error of at most 0.0003.
Values may be sent and summed in bfloat16 or wider, within the bound.
A program may use at most 128 MiB of HBM per device.

```python
import math
import jax
import jax.numpy as jnp

S = 16384
M = 96


def draw_gain_inverse(key, part):
    noise_key = jax.random.fold_in(key, 11)
    gains_key = jax.random.fold_in(key, 23)
    gains = jnp.exp(jax.random.uniform(gains_key, (S,), jnp.float32, jnp.log(0.6), jnp.log(1.6)))
    noise = jax.random.normal(noise_key, (S, S), jnp.float32)
    places = jnp.arange(S).astype(jnp.float32)
    distance = jnp.abs(places[:, None] - places[None, :])
    kernel = jnp.exp(-distance / (S / 4.0))
    ident = (distance == 0.0).astype(jnp.float32)
    rough = (noise + noise.T) * (0.4 / jnp.sqrt(2.0 * S))
    matrix = gains[:, None] * gains[None, :] * (ident + kernel + rough) / (2.0 * S)
    return matrix.astype(jnp.bfloat16)


def block_levels(own_key, dims, split, low, top_value):
    factor_of, own = 1.0, jax.random.fold_in(own_key, 6)
    for axis_at, parts in split:
        heights = jnp.exp(jax.random.uniform(jax.random.fold_in(own, axis_at), (parts,), jnp.float32, low / len(split), top_value / len(split)))
        factor_of = factor_of * jnp.repeat(heights, dims[axis_at] // parts).reshape([-1 if axis == axis_at else 1 for axis in range(len(dims))])
    return factor_of


def bell_draw(rng, extent, scale, reach, split=(), kind=jnp.bfloat16):
    drawn = jax.random.normal(rng, extent, jnp.float32) * scale
    if len(split) > 0:
        drawn = block_levels(rng, extent, split, -0.22, 0.18) * drawn
    return jnp.clip(drawn, min=-reach, max=reach).astype(kind)


def setup_inputs(seed: int = 0) -> dict:
    seeds = jax.random.split(jax.random.key(seed), 4)
    jacobian = bell_draw(seeds[0], (M, S), 1.0, 6.0, ((0, 32),))
    gain_inverse = draw_gain_inverse(jax.random.fold_in(seeds[3], 71), 0)
    variance = jnp.clip(jnp.exp(math.log(12.0) - 1.7917595 * jax.random.uniform(seeds[2], (M,), jnp.float32) ** block_levels(seeds[2], (M,), ((0, 32),), -0.2, 0.2)), 2.0, 12.0)
    return {"jacobian": jacobian, "gain_inverse": gain_inverse, "variance": variance}


def reference(jacobian, gain_inverse, variance):
    projected = jnp.dot(jacobian, gain_inverse, preferred_element_type=jnp.float32)
    quadratic = jnp.sum(projected * jacobian.astype(jnp.float32), axis=1)
    return variance - quadratic
```

```python
import functools

import jax
import jax.numpy as jnp
from jax import lax
from jax.experimental import pallas as pl
from jax.experimental.pallas import tpu as pltpu
from jax.sharding import PartitionSpec as P

LANES = 128
SUBLANES = 8
MESH = pl.DeviceIdType.MESH


def exchange_kernel(depth_count, blk_count, slots, *refs):
    count = len(slots)
    sources, targets = refs[:count], refs[count : 2 * count]
    send_sem, recv_sem, own_sem = refs[2 * count :]
    devices = depth_count * blk_count
    me = lax.axis_index("depth") * blk_count + lax.axis_index("blk")

    def place(device):
        return {"depth": device // blk_count, "blk": lax.rem(device, blk_count)}

    def peer(step):
        return lax.rem(me + step, devices)

    def slot_of(kind, device):
        if kind == "depth":
            return device // blk_count
        if kind == "blk":
            return lax.rem(device, blk_count)
        return device

    def copy(which, step):
        device = peer(step)
        return pltpu.make_async_remote_copy(
            src_ref=sources[which].at[slot_of(slots[which], device)],
            dst_ref=targets[which].at[me],
            send_sem=send_sem.at[which, step],
            recv_sem=recv_sem.at[which, step],
            device_id=place(device),
            device_id_type=MESH,
        )

    barrier = pltpu.get_barrier_semaphore()

    @pl.loop(1, devices)
    def _(step):
        pl.semaphore_signal(barrier, inc=1, device_id=place(peer(step)), device_id_type=MESH)

    own = [
        pltpu.make_async_copy(sources[w].at[slot_of(slots[w], me)], targets[w].at[me], own_sem.at[w])
        for w in range(count)
    ]
    for w in range(count):
        own[w].start()
    pl.semaphore_wait(barrier, devices - 1)

    @pl.loop(1, devices)
    def _(step):
        for w in range(count):
            copy(w, step).start()

    for w in range(count):
        own[w].wait()

    @pl.loop(1, devices)
    def _(step):
        for w in range(count):
            copy(w, step).wait()


def exchange(slots, collective_id, *operands):
    depth_count = lax.axis_size("depth")
    blk_count = lax.axis_size("blk")
    devices = depth_count * blk_count
    count = len(slots)
    vmem = pl.BlockSpec(memory_space=pltpu.VMEM)
    return pl.pallas_call(
        functools.partial(exchange_kernel, depth_count, blk_count, slots),
        out_shape=[jax.ShapeDtypeStruct((devices,) + x.shape[1:], x.dtype) for x in operands],
        in_specs=[vmem] * count,
        out_specs=[vmem] * count,
        scratch_shapes=[
            pltpu.SemaphoreType.DMA((count, devices)),
            pltpu.SemaphoreType.DMA((count, devices)),
            pltpu.SemaphoreType.DMA((count,)),
        ],
        compiler_params=pltpu.CompilerParams(collective_id=collective_id, has_side_effects=True),
    )(*operands)


def sections(jacobian, parts):
    rows, states = jacobian.shape
    width = states // parts
    return jacobian.reshape(rows, parts, width // LANES, LANES).transpose(1, 0, 2, 3)


def shards(jacobian, gain_inverse, variance):
    rows = jacobian.shape[0]
    depth_count = lax.axis_size("depth")
    blk_count = lax.axis_size("blk")
    devices = depth_count * blk_count
    left, right = exchange(
        ("depth", "blk"), 0, sections(jacobian, depth_count), sections(jacobian, blk_count)
    )
    left = left.reshape(devices * rows, -1)
    panel = right.reshape(devices * rows, -1)
    projected = jnp.dot(left, gain_inverse, preferred_element_type=jnp.float32)
    partial_sum = jnp.sum(projected * panel.astype(jnp.float32), axis=1)
    padded = jnp.pad(
        partial_sum.reshape(devices, 1, rows), ((0, 0), (0, SUBLANES - 1), (0, LANES - rows))
    )
    (gathered,) = exchange(("all",), 1, padded)
    quadratic = jnp.sum(gathered[:, 0, :rows], axis=0)
    return variance - quadratic


def solution(mesh):
    in_specs = (P(("depth", "blk"), None), P("depth", "blk"), P(("depth", "blk")))
    out_specs = P(("depth", "blk"))
    return jax.shard_map(shards, mesh=mesh, in_specs=in_specs, out_specs=out_specs, check_vma=False)
```
